256 devices in a mesh: band: 8 (over x, y_lo), grid: 32 (over y_hi, z, core).
Axes of the slice: x: 4, y: 4 (y_hi: 2, y_lo: 2; y = y_hi * 2 + y_lo), z: 8, core: 2. Of those that a mesh axis runs over, the one named last changes fastest.
Arguments:
- wavefunctions: bfloat16 [2048, 524288], P('band', 'grid'), may hold values from -6 to 6
- projectors: bfloat16 [2048, 8, 13, 256], P('grid'), may hold values from -0.0048828125 to 0.0048828125
- slot_atom: int32 [2048, 8], P('grid'), may hold values from -1 to 1023, as said below
- occupations: float32 [2048], P('band'), may hold values from 0.02 to 2
Outputs:
- density: float32 [1024, 13, 13], P('grid')
The draws below stay inside these ranges and needn't reach their ends.
Inputs may be any that keep to these rules, and one draw needn't show every extreme that they name: `slot_atom`: -1 marks an empty slot. Any other entry is an atom a whose owning domain a // 32 lies within 3 domains, counted around the closed cycle of 32 domains, of the domain of the block, block index // 64. In every domain some block has all 8 slots filled.
All inputs are finite; a program needn't handle non-finite values.
Results may differ from the reference program's by a relative error of at most 0.0003.
Values sent between devices are 32-bit elements; how exact they have to be, the bound alone decides.
A program may use at most 64 MiB of HBM per device.

```python
import math
import jax
import jax.numpy as jnp
from jax import lax

NPROJ = 13
BLK = 256
CAP = 8
REACH = 3
NBLK = 64
ATOMS_DEV = 32
BANDS = 2048
ATOMS = 1024
BLOCKS = 2048
POINTS = 524288
N_GRID = 32


def draw_slot_atom(key, part):
    keys = jax.random.split(jax.random.fold_in(key, 71), 6)
    domain = jnp.arange(BLOCKS, dtype=jnp.int32) // NBLK
    lowest = max(CAP // 3, 1)
    crowding = jax.random.randint(keys[0], (N_GRID,), lowest, CAP + 1)
    filled = jax.random.randint(keys[1], (BLOCKS,), 0, 1 << 20) % crowding[domain] + 1
    full_block = jax.random.randint(keys[2], (N_GRID,), 0, NBLK)
    is_full = jnp.arange(BLOCKS, dtype=jnp.int32) % NBLK == full_block[domain]
    filled = jnp.where(is_full, CAP, filled)
    scores = jax.random.randint(keys[3], (BLOCKS, CAP), 0, 1 << 16) * CAP + jnp.arange(CAP, dtype=jnp.int32)[None, :]
    ranking = jnp.argsort(jnp.argsort(scores, axis=1), axis=1)
    used = ranking < filled[:, None]
    offset = jax.random.randint(keys[4], (BLOCKS, CAP), -REACH, REACH + 1)
    owner = jnp.mod(domain[:, None] + offset, N_GRID)
    local_atom = jax.random.randint(keys[5], (BLOCKS, CAP), 0, ATOMS_DEV)
    return jnp.where(used, owner * ATOMS_DEV + local_atom, -1).astype(jnp.int32)


def block_levels(own_key, shape, shards, low, largest):
    def one(position, shards_of):
        heights = jax.random.uniform(jax.random.fold_in(jax.random.fold_in(own_key, 6), position), (shards_of,), jnp.float32, low / len(shards), largest / len(shards))
        return jnp.repeat(jnp.exp(heights), shape[position] // shards_of).reshape((-1,) + (1,) * (len(shape) - position - 1))

    gain = one(*shards[0])
    for cut in shards[1:]:
        gain = gain * one(*cut)
    return gain


def gaussian(rng, extent, deviation, bound, shards=(), kind=jnp.bfloat16):
    level = block_levels(rng, extent, shards, -0.22, 0.18) if shards else 1.0
    array = jax.random.normal(rng, extent, jnp.float32) * deviation * level
    return jnp.minimum(jnp.maximum(array, -bound), bound).astype(kind)


def setup_inputs(seed: int = 0) -> dict:
    seeds = jax.random.split(jax.random.key(seed), 5)
    wavefunctions = gaussian(seeds[0], (BANDS, POINTS), 1.0, 6.0, ((0, 8), (1, 32)))
    projectors = gaussian(seeds[1], (BLOCKS, CAP, NPROJ, BLK), (BANDS * NBLK * CAP * BLK // (6 * ATOMS_DEV)) ** -0.5, 0.0048828125, ((0, 32),))
    slot_atom = draw_slot_atom(jax.random.fold_in(seeds[4], 71), 0)
    occupations = jnp.clip(jnp.exp(math.log(2.0) - 4.6051702 * jax.random.uniform(seeds[3], (BANDS,), jnp.float32) ** block_levels(seeds[3], (BANDS,), ((0, 8),), -0.2, 0.2)), 0.02, 2.0)
    return dict(wavefunctions=wavefunctions, projectors=projectors, slot_atom=slot_atom, occupations=occupations)


def reference(wavefunctions, projectors, slot_atom, occupations):
    band_total = wavefunctions.shape[0]
    domain_points = NBLK * BLK

    def domain_step(running, domain):
        columns = lax.dynamic_slice_in_dim(wavefunctions, (domain * domain_points).astype(jnp.int32), domain_points, 1)
        pieces = lax.dynamic_slice_in_dim(projectors, (domain * NBLK).astype(jnp.int32), NBLK, 0)
        slot_ids = lax.dynamic_slice_in_dim(slot_atom, (domain * NBLK).astype(jnp.int32), NBLK, 0).reshape(-1)
        grid_blocks = columns.astype(jnp.float32).reshape(band_total, NBLK, BLK)
        stacked = pieces.astype(jnp.float32).reshape(NBLK, CAP * NPROJ, BLK)
        slot_terms = jnp.einsum("ngb,gcb->gcn", grid_blocks, stacked, precision=lax.Precision.HIGHEST)
        slot_terms = slot_terms.reshape(NBLK * CAP, NPROJ * band_total)
        target = jnp.where(slot_ids >= 0, slot_ids, ATOMS).astype(jnp.int32)
        running = running + jax.ops.segment_sum(slot_terms, target, num_segments=ATOMS + 1)
        return running, None

    initial = jnp.zeros((ATOMS + 1, NPROJ * band_total), jnp.float32)
    running, unused = lax.scan(domain_step, initial, jnp.arange(N_GRID, dtype=jnp.int32))
    projections = running[:ATOMS].reshape(ATOMS, NPROJ, band_total)
    weighted = projections * occupations.reshape(1, 1, band_total)
    return jnp.einsum("ain,ajn->aij", weighted, projections, precision=lax.Precision.HIGHEST)
```

```python
import functools

import jax
import jax.numpy as jnp
from jax import lax
from jax.experimental import pallas as pl
from jax.experimental.pallas import tpu as pltpu
from jax.sharding import PartitionSpec as P

REACH = 3
ATOMS_DEV = 32
NPROJ = 13
CAP = 8
NBLK = 64
BLK = 256
HALF = 128
WINDOW = 2 * REACH + 1
SLOTS = NBLK * CAP
GROUPS = ATOMS_DEV // 8
PIECES = 4
NT = (((1,), (1,)), ((), ()))
MESH = pl.DeviceIdType.MESH


def kernel(n_band, n_grid, target, occ, proj_hbm, wave_hbm, out, proj, wave, pick, high, low, window,
           landed, mine, gathered, proj_sem, wave_sem, send_sem, recv_sem, dsend_sem, drecv_sem):
    band = lax.axis_index("band")
    grid = lax.axis_index("grid")
    after = lax.rem(grid + 1, n_grid)
    before = lax.rem(grid + n_grid - 1, n_grid)

    barrier = pltpu.get_barrier_semaphore()
    for other in (after, before):
        pl.semaphore_signal(barrier, inc=1, device_id={"grid": other}, device_id_type=MESH)
    for step in range(1, n_band):
        pl.semaphore_signal(
            barrier, inc=1, device_id={"band": lax.rem(band + step, n_band)}, device_id_type=MESH
        )

    blocks = NBLK // PIECES
    cols = blocks * BLK
    proj_in, wave_in = [], [[], []]
    for k in range(PIECES):
        at = pl.ds(k * blocks, blocks)
        proj_in.append(pltpu.make_async_copy(proj_hbm.at[at], proj.at[at], proj_sem.at[k]))
    for h in range(2):
        for k in range(PIECES):
            at = (pl.ds(h * HALF, HALF), pl.ds(k * cols, cols))
            wave_in[h].append(pltpu.make_async_copy(wave_hbm.at[at], wave.at[at], wave_sem.at[h, k]))
    for k in range(PIECES):
        proj_in[k].start()
        wave_in[0][k].start()
    for k in range(PIECES):
        wave_in[1][k].start()

    rows = lax.broadcasted_iota(jnp.int32, (WINDOW * ATOMS_DEV, SLOTS), 0)
    pick[...] = jnp.where(rows == target[...], 1.0, 0.0).astype(jnp.bfloat16)

    def project(h):
        def two_blocks(pair):
            parts = []
            for g in (2 * pair, 2 * pair + 1):
                piece = wave[pl.ds(h * HALF, HALF), pl.ds(pl.multiple_of(g * BLK, BLK), BLK)]
                terms = lax.dot_general(proj[g], piece, NT, preferred_element_type=jnp.float32)
                parts.append(terms.reshape(NPROJ, CAP, HALF))
            terms = jnp.concatenate(parts, axis=1)
            top = terms.astype(jnp.bfloat16)
            rest = (terms - top.astype(jnp.float32)).astype(jnp.bfloat16)
            at = pl.ds(pl.multiple_of(pair * 16, 16), 16)
            for i in range(NPROJ):
                lanes = pl.ds(i % 2 * HALF, HALF)
                high[i // 2, at, lanes] = top[i]
                low[i // 2, at, lanes] = rest[i]

        for k in range(PIECES):
            if h == 0:
                proj_in[k].wait()
            wave_in[h][k].wait()

            def some(step, carry):
                for u in range(4):
                    two_blocks(k * (blocks // 2) + step * 4 + u)
                return carry

            lax.fori_loop(0, blocks // 8, some, 0)

    def select(h):
        for two in range((NPROJ + 1) // 2):
            width = 2 * HALF if two < NPROJ // 2 else HALF
            rows = jnp.dot(pick[...], high[two, :, :width], preferred_element_type=jnp.float32)
            rows += jnp.dot(pick[...], low[two, :, :width], preferred_element_type=jnp.float32)
            rows = rows.reshape(WINDOW * GROUPS, 8, width)
            for part in range(width // HALF):
                window[h, :, 2 * two + part] = rows[:, :, part * HALF:(part + 1) * HALF]

    def chunk(place, a):
        return pl.ds(place * GROUPS + 2 * a, 2)

    def send(phase, h, a, way):
        q = 2 * h + a
        place = 2 * phase + way
        return pltpu.make_async_remote_copy(
            src_ref=window.at[h, chunk(place, a)],
            dst_ref=landed.at[way, phase, q],
            send_sem=send_sem.at[way, phase, q],
            recv_sem=recv_sem.at[way, phase, q],
            device_id={"grid": after if way == 0 else before},
            device_id_type=MESH,
        )

    for h in range(2):
        project(h)
        select(h)
        if h == 0:
            pl.semaphore_wait(barrier, n_band + 1)
        for a in range(2):
            for way in range(2):
                send(0, h, a, way).start()

    for phase in (1, 2):
        for h in range(2):
            for a in range(2):
                for way in range(2):
                    send(phase - 1, h, a, way).wait_recv()
                    at = chunk(2 * phase + way, a)
                    window[h, at] = window[h, at] + landed[way, phase - 1, 2 * h + a]
                    send(phase, h, a, way).start()

    def share(step, a):
        other = lax.rem(band + step, n_band)
        return pltpu.make_async_remote_copy(
            src_ref=mine.at[a],
            dst_ref=gathered.at[n_band - 1 - step, a],
            send_sem=dsend_sem.at[step - 1, a],
            recv_sem=drecv_sem.at[step - 1, a],
            device_id={"band": other},
            device_id_type=MESH,
        )

    atom_of_row = lax.broadcasted_iota(jnp.int32, (NPROJ, 8, NPROJ * 8), 1)
    atom_of_lane = lax.broadcasted_iota(jnp.int32, (NPROJ, 8, NPROJ * 8), 2) % 8
    for h in range(2):
        weight = occ[:, h * HALF:(h + 1) * HALF]
        for a in range(2):
            q = 2 * h + a
            for way in range(2):
                send(2, h, a, way).wait_recv()
            for part in range(2):
                owned = window[h, 6 * GROUPS + 2 * a + part] + (landed[0, 2, q, part] + landed[1, 2, q, part])
                owned = owned.reshape(NPROJ * 8, HALF)
                gram = lax.dot_general(
                    owned, owned * weight, NT, precision=lax.Precision.HIGHEST,
                    preferred_element_type=jnp.float32,
                ).reshape(NPROJ, 8, NPROJ * 8)
                dens = jnp.sum(jnp.where(atom_of_row == atom_of_lane, gram, 0.0), axis=1)
                at = (a, part, slice(0, NPROJ), slice(0, NPROJ * 8))
                if h == 0:
                    mine[at] = dens
                else:
                    mine[at] = mine[at] + dens
            if h == 1:
                for step in range(1, n_band):
                    share(step, a).start()

    for a in range(2):
        for step in range(1, n_band):
            share(step, a).wait_recv()
        total = mine[a]
        for step in range(1, n_band):
            total = total + gathered[n_band - 1 - step, a]
        for i in range(NPROJ):
            for part in range(2):
                group = 2 * a + part
                out[i, :, group * 8:(group + 1) * 8] = total[part, :NPROJ, i * 8:(i + 1) * 8]

    for phase in range(3):
        for h in range(2):
            for a in range(2):
                for way in range(2):
                    send(phase, h, a, way).wait_send()
    for a in range(2):
        for step in range(1, n_band):
            share(step, a).wait_send()


def body(wavefunctions, projectors, slot_atom, occupations):
    n_band = lax.axis_size("band")
    n_grid = lax.axis_size("grid")
    domain = lax.axis_index("grid")
    stacked = jnp.transpose(projectors, (0, 2, 1, 3)).reshape(NBLK, NPROJ * CAP, BLK)
    offset = jnp.mod(jnp.floor_divide(slot_atom, ATOMS_DEV) - domain + REACH, n_grid)
    place = jnp.where(offset > REACH, 2 * (2 * REACH - offset), 2 * offset + 1)
    place = jnp.where(offset == REACH, 2 * REACH, place)
    target = jnp.where(slot_atom >= 0, place * ATOMS_DEV + jnp.mod(slot_atom, ATOMS_DEV), -1)
    vmem = pl.BlockSpec(memory_space=pltpu.VMEM)
    hbm = pl.BlockSpec(memory_space=pl.ANY)
    chunk = (2, NPROJ, 8, HALF)
    density = pl.pallas_call(
        functools.partial(kernel, n_band, n_grid),
        out_shape=jax.ShapeDtypeStruct((NPROJ, NPROJ, ATOMS_DEV), jnp.float32),
        in_specs=[vmem, vmem, hbm, hbm],
        out_specs=vmem,
        scratch_shapes=[
            pltpu.VMEM((NBLK, NPROJ * CAP, BLK), jnp.bfloat16),
            pltpu.VMEM((2 * HALF, NBLK * BLK), jnp.bfloat16),
            pltpu.VMEM((WINDOW * ATOMS_DEV, SLOTS), jnp.bfloat16),
            pltpu.VMEM(((NPROJ + 1) // 2, SLOTS, 2 * HALF), jnp.bfloat16),
            pltpu.VMEM(((NPROJ + 1) // 2, SLOTS, 2 * HALF), jnp.bfloat16),
            pltpu.VMEM((2, WINDOW * GROUPS, NPROJ, 8, HALF), jnp.float32),
            pltpu.VMEM((2, 3, 4) + chunk, jnp.float32),
            pltpu.VMEM((2, 2, 16, 128), jnp.float32),
            pltpu.VMEM((n_band - 1, 2, 2, 16, 128), jnp.float32),
            pltpu.SemaphoreType.DMA((PIECES,)),
            pltpu.SemaphoreType.DMA((2, PIECES)),
            pltpu.SemaphoreType.DMA((2, 3, 4)),
            pltpu.SemaphoreType.DMA((2, 3, 4)),
            pltpu.SemaphoreType.DMA((n_band - 1, 2)),
            pltpu.SemaphoreType.DMA((n_band - 1, 2)),
        ],
        compiler_params=pltpu.CompilerParams(collective_id=0, has_side_effects=True),
        name="density",
    )(target.reshape(1, SLOTS), occupations.reshape(1, 2 * HALF), stacked, wavefunctions)
    return jnp.transpose(density, (2, 0, 1))


def solution(mesh):
    in_specs = (P("band", "grid"), P("grid", None, None, None), P("grid", None), P("band"))
    out_specs = P("grid", None, None)
    return jax.shard_map(body, mesh=mesh, in_specs=in_specs, out_specs=out_specs, check_vma=False)
```

```python
import functools

import jax
import jax.numpy as jnp
from jax import lax
from jax.experimental import pallas as pl
from jax.experimental.pallas import tpu as pltpu
from jax.sharding import PartitionSpec as P

REACH = 3
ATOMS_DEV = 32
NPROJ = 13
CAP = 8
NBLK = 64
BLK = 256
HALF = 128
WINDOW = 2 * REACH + 1
SLOTS = NBLK * CAP
GROUPS = ATOMS_DEV // 8
VMEM_LIMIT = 55000000
AHEAD = 2
PIECES = 4
NT = (((1,), (1,)), ((), ()))
MESH = pl.DeviceIdType.MESH


def kernel(n_band, n_grid, slot_hbm, occ_hbm, proj_hbm, wave_hbm, out, slot, occ, proj, wave, pick, high, low, window,
           landed, mine, gathered, small_sem, proj_sem, wave_sem, send_sem, recv_sem, dsend_sem, drecv_sem):
    band = lax.axis_index("band")
    grid = lax.axis_index("grid")
    after = lax.rem(grid + 1, n_grid)
    before = lax.rem(grid + n_grid - 1, n_grid)

    barrier = pltpu.get_barrier_semaphore()
    for other in (after, before):
        pl.semaphore_signal(barrier, inc=1, device_id={"grid": other}, device_id_type=MESH)
    for step in range(1, n_band):
        pl.semaphore_signal(
            barrier, inc=1, device_id={"band": lax.rem(band + step, n_band)}, device_id_type=MESH
        )

    blocks = NBLK // PIECES
    cols = blocks * BLK
    proj_in, wave_in = [], [[], []]
    for k in range(PIECES):
        at = pl.ds(k * blocks, blocks)
        proj_in.append(pltpu.make_async_copy(proj_hbm.at[at], proj.at[at], proj_sem.at[k]))
    for h in range(2):
        for k in range(PIECES):
            at = (pl.ds(h * HALF, HALF), pl.ds(k * cols, cols))
            wave_in[h].append(pltpu.make_async_copy(wave_hbm.at[at], wave.at[at], wave_sem.at[h, k]))
    slot_in = pltpu.make_async_copy(slot_hbm, slot, small_sem.at[0])
    occ_in = pltpu.make_async_copy(occ_hbm, occ, small_sem.at[1])
    slot_in.start()
    loads = [[proj_in[k], wave_in[0][k]] for k in range(PIECES)] + [[wave_in[1][k]] for k in range(PIECES)]
    loads[-1].append(occ_in)
    for copies in loads[:AHEAD]:
        for copy in copies:
            copy.start()

    slot_in.wait()
    ids = slot[...]
    offset = (ids >> 5) - grid
    offset = jnp.where(offset > n_grid // 2, offset - n_grid, offset)
    offset = jnp.where(offset < -(n_grid // 2), offset + n_grid, offset)
    place = jnp.where(offset > 0, 2 * (REACH - offset), 2 * (REACH + offset) + 1)
    place = jnp.where(offset == 0, 2 * REACH, place)
    target = jnp.where(ids >= 0, place * ATOMS_DEV + (ids & (ATOMS_DEV - 1)), -1)
    spread = lax.broadcasted_iota(jnp.int32, (NBLK, SLOTS), 1) >> 3
    spread = (spread == lax.broadcasted_iota(jnp.int32, (NBLK, SLOTS), 0)).astype(jnp.float32)
    target = jnp.dot(
        target.astype(jnp.float32).astype(jnp.bfloat16), spread.astype(jnp.bfloat16),
        preferred_element_type=jnp.float32,
    )
    own_slot = (lax.broadcasted_iota(jnp.int32, (CAP, SLOTS), 1) & 7) == lax.broadcasted_iota(
        jnp.int32, (CAP, SLOTS), 0
    )
    target = jnp.sum(jnp.where(own_slot, target, 0.0), axis=0, keepdims=True).astype(jnp.int32)
    rows = lax.broadcasted_iota(jnp.int32, (WINDOW * ATOMS_DEV, SLOTS), 0)
    pick[...] = jnp.where(rows == target, 1.0, 0.0).astype(jnp.bfloat16)

    def project(h):
        def two_blocks(pair):
            parts = []
            for g in (2 * pair, 2 * pair + 1):
                piece = wave[pl.ds(h * HALF, HALF), pl.ds(g * BLK, BLK)]
                terms = lax.dot_general(proj[g], piece, NT, preferred_element_type=jnp.float32)
                parts.append(terms.reshape(NPROJ, CAP, HALF))
            terms = jnp.concatenate(parts, axis=1)
            top = terms.astype(jnp.bfloat16)
            rest = (terms - top.astype(jnp.float32)).astype(jnp.bfloat16)
            at = pl.ds(pair * 16, 16)
            for i in range(NPROJ):
                lanes = pl.ds(i % 2 * HALF, HALF)
                high[i // 2, at, lanes] = top[i]
                low[i // 2, at, lanes] = rest[i]

        for k in range(PIECES):
            turn = h * PIECES + k
            for copy in loads[turn]:
                copy.wait()
            for copy in loads[turn + AHEAD] if turn + AHEAD < len(loads) else ():
                copy.start()
            for pair in range(blocks // 2):
                two_blocks(k * (blocks // 2) + pair)
            if k % 2 == 1:
                select(h, k // 2)

    def select(h, part):
        at = slice(part * SLOTS // 2, (part + 1) * SLOTS // 2)
        for two in range((NPROJ + 1) // 2):
            width = 2 * HALF if two < NPROJ // 2 else HALF
            rows = jnp.dot(pick[:, at], high[two, at, :width], preferred_element_type=jnp.float32)
            rows += jnp.dot(pick[:, at], low[two, at, :width], preferred_element_type=jnp.float32)
            rows = rows.reshape(WINDOW * GROUPS, 8, width)
            for lane in range(width // HALF):
                i = 2 * two + lane
                sums = rows[:, :, lane * HALF:(lane + 1) * HALF]
                window[h, :, i] = sums if part == 0 else window[h, :, i] + sums

    def chunk(place, a):
        return pl.ds(place * GROUPS + 2 * a, 2)

    def send(phase, h, a, way):
        q = 2 * h + a
        place = 2 * phase + way
        return pltpu.make_async_remote_copy(
            src_ref=window.at[h, chunk(place, a)],
            dst_ref=landed.at[way, phase, q],
            send_sem=send_sem.at[way, phase, q],
            recv_sem=recv_sem.at[way, phase, q],
            device_id={"grid": after if way == 0 else before},
            device_id_type=MESH,
        )

    for h in range(2):
        project(h)
        if h == 0:
            pl.semaphore_wait(barrier, n_band + 1)
        for a in range(2):
            for way in range(2):
                send(0, h, a, way).start()

    for phase in (1, 2):
        for h in range(2):
            for a in range(2):
                for way in range(2):
                    send(phase - 1, h, a, way).wait_recv()
                    at = chunk(2 * phase + way, a)
                    window[h, at] = window[h, at] + landed[way, phase - 1, 2 * h + a]
                    send(phase, h, a, way).start()

    def share(step, a):
        other = lax.rem(band + step, n_band)
        return pltpu.make_async_remote_copy(
            src_ref=mine.at[a],
            dst_ref=gathered.at[n_band - 1 - step, a],
            send_sem=dsend_sem.at[step - 1, a],
            recv_sem=drecv_sem.at[step - 1, a],
            device_id={"band": other},
            device_id_type=MESH,
        )

    atom_of_row = lax.broadcasted_iota(jnp.int32, (NPROJ, 8, NPROJ * 8), 1)
    atom_of_lane = lax.broadcasted_iota(jnp.int32, (NPROJ, 8, NPROJ * 8), 2) % 8
    for h in range(2):
        weight = occ[:, h * HALF:(h + 1) * HALF]
        for a in range(2):
            q = 2 * h + a
            for way in range(2):
                send(2, h, a, way).wait_recv()
            for part in range(2):
                owned = window[h, 6 * GROUPS + 2 * a + part] + (landed[0, 2, q, part] + landed[1, 2, q, part])
                owned = owned.reshape(NPROJ * 8, HALF)
                gram = lax.dot_general(
                    owned, owned * weight, NT, precision=lax.Precision.HIGHEST,
                    preferred_element_type=jnp.float32,
                ).reshape(NPROJ, 8, NPROJ * 8)
                dens = jnp.sum(jnp.where(atom_of_row == atom_of_lane, gram, 0.0), axis=1)
                at = (a, part, slice(0, NPROJ), slice(0, NPROJ * 8))
                if h == 0:
                    mine[at] = dens
                else:
                    mine[at] = mine[at] + dens
            if h == 1:
                for step in range(1, n_band):
                    share(step, a).start()

    for a in range(2):
        for step in range(1, n_band):
            share(step, a).wait_recv()
        total = mine[a]
        for step in range(1, n_band):
            total = total + gathered[n_band - 1 - step, a]
        for i in range(NPROJ):
            for part in range(2):
                group = 2 * a + part
                out[i, :, group * 8:(group + 1) * 8] = total[part, :NPROJ, i * 8:(i + 1) * 8]

    for phase in range(3):
        for h in range(2):
            for a in range(2):
                for way in range(2):
                    send(phase, h, a, way).wait_send()
    for a in range(2):
        for step in range(1, n_band):
            share(step, a).wait_send()


def body(wavefunctions, projectors, slot_atom, occupations):
    n_band = lax.axis_size("band")
    n_grid = lax.axis_size("grid")
    stacked = jnp.transpose(projectors, (0, 2, 1, 3)).reshape(NBLK, NPROJ * CAP, BLK)
    vmem = pl.BlockSpec(memory_space=pltpu.VMEM)
    hbm = pl.BlockSpec(memory_space=pltpu.HBM)
    chunk = (2, NPROJ, 8, HALF)
    density = pl.pallas_call(
        functools.partial(kernel, n_band, n_grid),
        out_shape=jax.ShapeDtypeStruct((NPROJ, NPROJ, ATOMS_DEV), jnp.float32),
        in_specs=[hbm] * 4,
        out_specs=vmem,
        scratch_shapes=[
            pltpu.VMEM((CAP, NBLK), jnp.int32),
            pltpu.VMEM((1, 2 * HALF), jnp.float32),
            pltpu.VMEM((NBLK, NPROJ * CAP, BLK), jnp.bfloat16),
            pltpu.VMEM((2 * HALF, NBLK * BLK), jnp.bfloat16),
            pltpu.VMEM((WINDOW * ATOMS_DEV, SLOTS), jnp.bfloat16),
            pltpu.VMEM(((NPROJ + 1) // 2, SLOTS, 2 * HALF), jnp.bfloat16),
            pltpu.VMEM(((NPROJ + 1) // 2, SLOTS, 2 * HALF), jnp.bfloat16),
            pltpu.VMEM((2, WINDOW * GROUPS, NPROJ, 8, HALF), jnp.float32),
            pltpu.VMEM((2, 3, 4) + chunk, jnp.float32),
            pltpu.VMEM((2, 2, 16, 128), jnp.float32),
            pltpu.VMEM((n_band - 1, 2, 2, 16, 128), jnp.float32),
            pltpu.SemaphoreType.DMA((2,)),
            pltpu.SemaphoreType.DMA((PIECES,)),
            pltpu.SemaphoreType.DMA((2, PIECES)),
            pltpu.SemaphoreType.DMA((2, 3, 4)),
            pltpu.SemaphoreType.DMA((2, 3, 4)),
            pltpu.SemaphoreType.DMA((n_band - 1, 2)),
            pltpu.SemaphoreType.DMA((n_band - 1, 2)),
        ],
        compiler_params=pltpu.CompilerParams(collective_id=0, has_side_effects=True, vmem_limit_bytes=VMEM_LIMIT),
        name="density",
    )(*(pltpu.with_memory_space_constraint(x, pltpu.HBM) for x in (slot_atom.T, occupations.reshape(1, 2 * HALF), stacked, wavefunctions)))
    return jnp.transpose(density, (2, 0, 1))


def solution(mesh):
    in_specs = (P("band", "grid"), P("grid", None, None, None), P("grid", None), P("band"))
    out_specs = P("grid", None, None)
    return jax.shard_map(body, mesh=mesh, in_specs=in_specs, out_specs=out_specs, check_vma=False)
```

```python
import functools

import jax
import jax.numpy as jnp
from jax import lax
from jax.experimental import pallas as pl
from jax.experimental.pallas import tpu as pltpu
from jax.sharding import PartitionSpec as P

REACH = 3
ATOMS_DEV = 32
NPROJ = 13
CAP = 8
NBLK = 64
BLK = 256
HALF = 128
WINDOW = 2 * REACH + 1
SLOTS = NBLK * CAP
GROUPS = ATOMS_DEV // 8
VMEM_LIMIT = 55000000
AHEAD = (3, 0, 1, 1, 0)
PIECES = ((12, 20, 32), (64,))
NT = (((1,), (1,)), ((), ()))
MESH = pl.DeviceIdType.MESH


def kernel(n_band, n_grid, slot_hbm, occ_hbm, proj_hbm, wave_hbm, out, slot, occ, proj, wave, pick, high, low, window,
           landed, mine, gathered, small_sem, proj_sem, wave_sem, send_sem, recv_sem, lsend_sem, lrecv_sem,
           dsend_sem, drecv_sem):
    band = lax.axis_index("band")
    grid = lax.axis_index("grid")
    after = lax.rem(grid + 1, n_grid)
    before = lax.rem(grid + n_grid - 1, n_grid)

    barrier = pltpu.get_barrier_semaphore()
    for other in (after, before):
        pl.semaphore_signal(barrier, inc=1, device_id={"grid": other}, device_id_type=MESH)
    for step in range(1, n_band):
        pl.semaphore_signal(
            barrier, inc=1, device_id={"band": lax.rem(band + step, n_band)}, device_id_type=MESH
        )

    slot_in = pltpu.make_async_copy(slot_hbm, slot, small_sem.at[0])
    occ_in = pltpu.make_async_copy(occ_hbm, occ, small_sem.at[1])
    slot_in.start()
    loads = []
    for h in range(2):
        first = 0
        for k, blocks in enumerate(PIECES[h]):
            at = pl.ds(first, blocks)
            cols = (pl.ds(h * HALF, HALF), pl.ds(first * BLK, blocks * BLK))
            copies = [pltpu.make_async_copy(wave_hbm.at[cols], wave.at[cols], wave_sem.at[h, k])]
            if h == 0:
                copies.append(pltpu.make_async_copy(proj_hbm.at[at], proj.at[at], proj_sem.at[k]))
            loads.append((first, blocks, copies))
            first += blocks
    loads[-1][2].append(occ_in)
    waiting = list(loads)

    def issue(count):
        for _ in range(min(count, len(waiting))):
            first, blocks, copies = waiting.pop(0)
            for copy in copies:
                copy.start(priority=int(len(waiting) < len(PIECES[1])))

    issue(AHEAD[0])

    slot_in.wait()
    ids = slot[...]
    offset = (ids >> 5) - grid
    offset = jnp.where(offset > n_grid // 2, offset - n_grid, offset)
    offset = jnp.where(offset < -(n_grid // 2), offset + n_grid, offset)
    place = jnp.where(offset > 0, 2 * (REACH - offset), 2 * (REACH + offset) + 1)
    place = jnp.where(offset == 0, 2 * REACH, place)
    target = jnp.where(ids >= 0, place * ATOMS_DEV + (ids & (ATOMS_DEV - 1)), -1)
    spread = lax.broadcasted_iota(jnp.int32, (NBLK, SLOTS), 1) >> 3
    spread = (spread == lax.broadcasted_iota(jnp.int32, (NBLK, SLOTS), 0)).astype(jnp.float32)
    target = jnp.dot(
        target.astype(jnp.float32).astype(jnp.bfloat16), spread.astype(jnp.bfloat16),
        preferred_element_type=jnp.float32,
    )
    own_slot = (lax.broadcasted_iota(jnp.int32, (CAP, SLOTS), 1) & 7) == lax.broadcasted_iota(
        jnp.int32, (CAP, SLOTS), 0
    )
    target = jnp.sum(jnp.where(own_slot, target, 0.0), axis=0, keepdims=True).astype(jnp.int32)
    rows = lax.broadcasted_iota(jnp.int32, (WINDOW * ATOMS_DEV, SLOTS), 0)
    pick[...] = jnp.where(rows == target, 1.0, 0.0).astype(jnp.bfloat16)

    def project(h):
        def two_blocks(pair):
            parts = []
            for g in (2 * pair, 2 * pair + 1):
                piece = wave[pl.ds(h * HALF, HALF), pl.ds(g * BLK, BLK)]
                terms = lax.dot_general(proj[g], piece, NT, preferred_element_type=jnp.float32)
                parts.append(terms.reshape(NPROJ, CAP, HALF))
            terms = jnp.concatenate(parts, axis=1)
            top = terms.astype(jnp.bfloat16)
            rest = (terms - top.astype(jnp.float32)).astype(jnp.bfloat16)
            at = pl.ds(pair * 16, 16)
            for i in range(NPROJ):
                lanes = pl.ds(i % 2 * HALF, HALF)
                high[i // 2, at, lanes] = top[i]
                low[i // 2, at, lanes] = rest[i]

        for k in range(len(PIECES[h])):
            turn = h * len(PIECES[0]) + k
            first, blocks, copies = loads[turn]
            for copy in copies:
                copy.wait()
            issue(AHEAD[turn + 1])
            for pair in range(first // 2, (first + blocks) // 2):
                two_blocks(pair)
                if pair % (NBLK // 4) == NBLK // 4 - 1:
                    select(h, pair // (NBLK // 4))

    def select(h, part):
        at = slice(part * SLOTS // 2, (part + 1) * SLOTS // 2)
        for two in range((NPROJ + 1) // 2):
            width = 2 * HALF if two < NPROJ // 2 else HALF
            rows = jnp.dot(pick[:, at], high[two, at, :width], preferred_element_type=jnp.float32)
            rows += jnp.dot(pick[:, at], low[two, at, :width], preferred_element_type=jnp.float32)
            rows = rows.reshape(WINDOW * GROUPS, 8, width)
            for lane in range(width // HALF):
                i = 2 * two + lane
                sums = rows[:, :, lane * HALF:(lane + 1) * HALF]
                window[h, :, i] = sums if part == 0 else window[h, :, i] + sums

    def chunk(place, a):
        return pl.ds(place * GROUPS + 2 * a, 2)

    def send(phase, h, a, way):
        q = 2 * h + a
        place = 2 * phase + way
        return pltpu.make_async_remote_copy(
            src_ref=window.at[h, chunk(place, a)],
            dst_ref=landed.at[way, phase, q],
            send_sem=send_sem.at[way, phase, q],
            recv_sem=recv_sem.at[way, phase, q],
            device_id={"grid": after if way == 0 else before},
            device_id_type=MESH,
        )

    def last(h, a, way, part):
        q = 2 * h + a
        return pltpu.make_async_remote_copy(
            src_ref=window.at[h, (4 + way) * GROUPS + 2 * a + part],
            dst_ref=landed.at[way, 2, q, part],
            send_sem=lsend_sem.at[way, q, part],
            recv_sem=lrecv_sem.at[way, q, part],
            device_id={"grid": after if way == 0 else before},
            device_id_type=MESH,
        )

    for h in range(2):
        project(h)
        if h == 0:
            pl.semaphore_wait(barrier, n_band + 1)
        for a in range(2):
            for way in range(2):
                send(0, h, a, way).start()

    for phase in (1, 2):
        for h in range(2):
            for a in range(2):
                for way in range(2):
                    send(phase - 1, h, a, way).wait_recv()
                    at = chunk(2 * phase + way, a)
                    window[h, at] = window[h, at] + landed[way, phase - 1, 2 * h + a]
                    if phase == 1:
                        send(phase, h, a, way).start()
                    else:
                        for part in range(2):
                            last(h, a, way, part).start()

    def share(step, a):
        other = lax.rem(band + step, n_band)
        return pltpu.make_async_remote_copy(
            src_ref=mine.at[a],
            dst_ref=gathered.at[n_band - 1 - step, a],
            send_sem=dsend_sem.at[step - 1, a],
            recv_sem=drecv_sem.at[step - 1, a],
            device_id={"band": other},
            device_id_type=MESH,
        )

    steps = sorted(range(1, n_band), key=lambda step: abs(step - n_band // 2))

    atom_of_row = lax.broadcasted_iota(jnp.int32, (NPROJ, 8, NPROJ * 8), 1)
    atom_of_lane = lax.broadcasted_iota(jnp.int32, (NPROJ, 8, NPROJ * 8), 2) % 8
    for h in range(2):
        weight = occ[:, h * HALF:(h + 1) * HALF]
        for a in range(2):
            q = 2 * h + a
            for part in range(2):
                for way in range(2):
                    last(h, a, way, part).wait_recv()
                owned = window[h, 6 * GROUPS + 2 * a + part] + (landed[0, 2, q, part] + landed[1, 2, q, part])
                owned = owned.reshape(NPROJ * 8, HALF)
                gram = lax.dot_general(
                    owned, owned * weight, NT, precision=lax.Precision.HIGHEST,
                    preferred_element_type=jnp.float32,
                ).reshape(NPROJ, 8, NPROJ * 8)
                dens = jnp.sum(jnp.where(atom_of_row == atom_of_lane, gram, 0.0), axis=1)
                at = (a, part, slice(0, NPROJ), slice(0, NPROJ * 8))
                if h == 0:
                    mine[at] = dens
                else:
                    mine[at] = mine[at] + dens
            if h == 1:
                for step in steps:
                    share(step, a).start()

    for a in range(2):
        for step in range(1, n_band):
            share(step, a).wait_recv()
        for part in range(2):
            total = mine[a, part]
            for step in range(1, n_band):
                total = total + gathered[n_band - 1 - step, a, part]
            group = 2 * a + part
            for i in range(NPROJ):
                out[i, :, group * 8:(group + 1) * 8] = total[:NPROJ, i * 8:(i + 1) * 8]

    for h in range(2):
        for a in range(2):
            for way in range(2):
                for phase in range(2):
                    send(phase, h, a, way).wait_send()
                for part in range(2):
                    last(h, a, way, part).wait_send()
    for a in range(2):
        for step in range(1, n_band):
            share(step, a).wait_send()


def body(wavefunctions, projectors, slot_atom, occupations):
    n_band = lax.axis_size("band")
    n_grid = lax.axis_size("grid")
    stacked = jnp.transpose(projectors, (0, 2, 1, 3)).reshape(NBLK, NPROJ * CAP, BLK)
    vmem = pl.BlockSpec(memory_space=pltpu.VMEM)
    hbm = pl.BlockSpec(memory_space=pltpu.HBM)
    chunk = (2, NPROJ, 8, HALF)
    density = pl.pallas_call(
        functools.partial(kernel, n_band, n_grid),
        out_shape=jax.ShapeDtypeStruct((NPROJ, NPROJ, ATOMS_DEV), jnp.float32),
        in_specs=[hbm] * 4,
        out_specs=vmem,
        scratch_shapes=[
            pltpu.VMEM((CAP, NBLK), jnp.int32),
            pltpu.VMEM((1, 2 * HALF), jnp.float32),
            pltpu.VMEM((NBLK, NPROJ * CAP, BLK), jnp.bfloat16),
            pltpu.VMEM((2 * HALF, NBLK * BLK), jnp.bfloat16),
            pltpu.VMEM((WINDOW * ATOMS_DEV, SLOTS), jnp.bfloat16),
            pltpu.VMEM(((NPROJ + 1) // 2, SLOTS, 2 * HALF), jnp.bfloat16),
            pltpu.VMEM(((NPROJ + 1) // 2, SLOTS, 2 * HALF), jnp.bfloat16),
            pltpu.VMEM((2, WINDOW * GROUPS, NPROJ, 8, HALF), jnp.float32),
            pltpu.VMEM((2, 3, 4) + chunk, jnp.float32),
            pltpu.VMEM((2, 2, 16, 128), jnp.float32),
            pltpu.VMEM((n_band - 1, 2, 2, 16, 128), jnp.float32),
            pltpu.SemaphoreType.DMA((2,)),
            pltpu.SemaphoreType.DMA((len(PIECES[0]),)),
            pltpu.SemaphoreType.DMA((2, max(len(p) for p in PIECES))),
            pltpu.SemaphoreType.DMA((2, 2, 4)),
            pltpu.SemaphoreType.DMA((2, 2, 4)),
            pltpu.SemaphoreType.DMA((2, 4, 2)),
            pltpu.SemaphoreType.DMA((2, 4, 2)),
            pltpu.SemaphoreType.DMA((n_band - 1, 2)),
            pltpu.SemaphoreType.DMA((n_band - 1, 2)),
        ],
        compiler_params=pltpu.CompilerParams(collective_id=0, has_side_effects=True, vmem_limit_bytes=VMEM_LIMIT),
        name="density",
    )(*(pltpu.with_memory_space_constraint(x, pltpu.HBM) for x in (slot_atom.T, occupations.reshape(1, 2 * HALF), stacked, wavefunctions)))
    return jnp.transpose(density, (2, 0, 1))


def solution(mesh):
    in_specs = (P("band", "grid"), P("grid", None, None, None), P("grid", None), P("band"))
    out_specs = P("grid", None, None)
    return jax.shard_map(body, mesh=mesh, in_specs=in_specs, out_specs=out_specs, check_vma=False)
```
